32 devices in a mesh: grp: 2 (over x), sub: 16 (over z, y, core).
Axes of the slice: x: 2, y: 2, z: 4, core: 2. Of those that a mesh axis runs over, the one named last changes fastest.
Arguments:
- counts: int32 [32], P(('grp', 'sub')), may hold values from 1 to 3, as said below
- block_map: int32 [96], P(('grp', 'sub')), may hold values from 0 to 31
- perms: int32 [96, 256], P(('grp', 'sub')), may hold values from 0 to 255, each once within a row
- mass_ii: bfloat16 [96, 1024, 1024], P(('grp', 'sub')), may hold values from -0.005859375 to 0.005859375
- mass_ib: bfloat16 [96, 1024, 256], P(('grp', 'sub')), may hold values from -0.1875 to 0.1875
- mass_bb: bfloat16 [96, 256, 256], P(('grp', 'sub')), may hold values from -6 to 6
- constraint_modes: bfloat16 [96, 1024, 256], P(('grp', 'sub')), may hold values from -6 to 6
- fixed_modes: bfloat16 [96, 1024, 128], P(('grp', 'sub')), may hold values from -6 to 6
Outputs:
- blocks: float32 [32, 256, 256], P('grp', 'sub')
- coupling: float32 [96, 128, 256], P(('grp', 'sub'))
The draws below stay inside these ranges and needn't reach their ends.
Inputs may be any that keep to these rules, and one draw needn't show every extreme that they name: `counts`: at least one device uses all 3 slots and one uses a single slot.
All inputs are finite; a program needn't handle non-finite values.
Results may differ from the reference program's by a relative error of at most 0.0021.
Values sent between devices are 32-bit elements; how exact they have to be, the bound alone decides.
No kernel may reach another device: no remote copies, remote signals or barrier semaphores. Data moves between devices by JAX's collectives and lax.ppermute only.
A program may use at most 128 MiB of HBM per device.

```python
import jax
import jax.numpy as jnp
from jax import lax

I = 1024
B = 256
K = 128
SLOTS = 3
NBG = 16
CAP = 96
N_GRP = 2
N_SUB = 16
DEVICES = 32


def draw_counts(key, part):
    raw = jax.random.randint(key, (DEVICES,), 0, 6)
    values = jnp.where(raw < 4, 1, jnp.where(raw == 4, 2, SLOTS))
    values = jnp.minimum(values, SLOTS)
    values = values.at[0].set(SLOTS).at[1].set(1)
    return values.astype(jnp.int32)


def place_ends(drawn, own_key, low, high):
    extent = drawn.shape
    place = [jax.random.randint(jax.random.fold_in(own_key, axis), (), 0, extent[axis]) for axis in range(len(extent))]
    drawn = drawn.at[tuple(place)].set(low)
    longest = extent.index(max(extent))
    place[longest] = (place[longest] + 1) % extent[longest]
    return drawn.at[tuple(place)].set(high)


def shard_levels(stream_key, shape, cuts, low, high):
    level, own = 1.0, jax.random.fold_in(stream_key, 6)
    for axis_at, parts in cuts:
        heights = jnp.exp(jax.random.uniform(jax.random.fold_in(own, axis_at), (parts,), jnp.float32, low / len(cuts), high / len(cuts)))
        level = level * jnp.repeat(heights, shape[axis_at] // parts).reshape([-1 if axis == axis_at else 1 for axis in range(len(shape))])
    return level


def scatter_about(key, extent, deviation, bound, shards=(), held_as=jnp.bfloat16):
    drawn = jax.random.normal(key, extent, jnp.float32) * deviation
    if len(shards) > 0:
        drawn = shard_levels(key, extent, shards, -0.22, 0.18) * drawn
    return jnp.clip(drawn, min=-bound, max=bound).astype(held_as)


def setup_inputs(seed: int = 0) -> dict:
    keys = jax.random.split(jax.random.key(seed), 9)
    return {
        "counts": draw_counts(jax.random.fold_in(keys[8], 71), 0),
        "block_map": place_ends(jax.random.randint(keys[1], (CAP,), 0, 2 * NBG), jax.random.fold_in(keys[1], 1), 0, (2 * NBG) - 1).astype(jnp.int32),
        "perms": jax.vmap(lambda own: jax.random.permutation(own, B))(jax.random.split(keys[2], CAP)).reshape((CAP, B)).astype(jnp.int32),
        "mass_ii": scatter_about(keys[3], (CAP, I, I), (I * I) ** -0.5, 0.005859375, ((0, 32),)),
        "mass_ib": scatter_about(keys[4], (CAP, I, B), I ** -0.5, 0.1875, ((0, 32),)),
        "mass_bb": scatter_about(keys[5], (CAP, B, B), 1.0, 6.0, ((0, 32),)),
        "constraint_modes": scatter_about(keys[6], (CAP, I, B), 1.0, 6.0, ((0, 32),)),
        "fixed_modes": scatter_about(keys[7], (CAP, I, K), 1.0, 6.0, ((0, 32),)),
    }


def contract(left, right):
    return lax.dot_general(left, right, (((0,), (0,)), ((), ())), preferred_element_type=jnp.float32)


def reduce_slot(mass_ii, mass_ib, mass_bb, constraint_modes, fixed_modes):
    product = jnp.dot(mass_ii, constraint_modes, preferred_element_type=jnp.float32).astype(jnp.bfloat16)
    cross = contract(constraint_modes, mass_ib)
    reduced = contract(constraint_modes, product) + cross + cross.T + mass_bb.astype(jnp.float32)
    coupled = contract(fixed_modes, product) + contract(fixed_modes, mass_ib)
    return reduced, coupled


def reference(counts, block_map, perms, mass_ii, mass_ib, mass_bb, constraint_modes, fixed_modes):
    width = mass_bb.shape[1]
    total_slots = mass_ii.shape[0]
    modes = fixed_modes.shape[2]

    def step(carry_blocks, items):
        slot_id, code, perm_row, m_ii, m_ib, m_bb, psi_slot, phi_slot = items
        device = slot_id // SLOTS
        used_flag = (slot_id % SLOTS) < counts[device]
        group_index = device // N_SUB

        def active_branch(unused):
            return reduce_slot(m_ii, m_ib, m_bb, psi_slot, phi_slot)

        def empty_branch(unused):
            return (jnp.zeros((width, width), jnp.float32), jnp.zeros((modes, width), jnp.float32))

        reduced, coupled = lax.cond(used_flag, active_branch, empty_branch, 0)
        target = ((group_index + code // NBG) % N_GRP) * NBG + code % NBG
        inverse = jnp.zeros((width,), jnp.int32).at[perm_row].set(jnp.arange(width, dtype=jnp.int32))
        placed = reduced[inverse][:, inverse]
        carry_blocks = carry_blocks.at[target.astype(jnp.int32)].add(placed)
        return carry_blocks, coupled

    start = jnp.zeros((NBG * N_GRP, width, width), jnp.float32)
    items = (jnp.arange(total_slots, dtype=jnp.int32), block_map, perms, mass_ii, mass_ib, mass_bb, constraint_modes, fixed_modes)
    blocks, coupling = lax.scan(step, start, items)
    return blocks, coupling
```

```python
import functools

import jax
import jax.numpy as jnp
from jax import lax
from jax.experimental import pallas as pl
from jax.experimental.pallas import tpu as pltpu
from jax.sharding import PartitionSpec as P

NBG = 16
OUTER = 4
META = 8
F32 = jnp.float32
BF16 = jnp.bfloat16


def shifted(value, axis, by):
    peers = lax.axis_size(axis)
    return lax.ppermute(value, axis, [(i, (i + by) % peers) for i in range(peers)])


def crossed(value, mask):
    peers = lax.axis_size("sub")
    return lax.ppermute(value, "sub", [(i, i ^ mask) for i in range(peers)])


def mm(left, right, dims):
    return lax.dot_general(left, right, (dims, ((), ())), preferred_element_type=F32)


def halves(value):
    high = value.astype(BF16)
    return high, (value - high.astype(F32)).astype(BF16)


def slot_body(slot, inner, outer, rows, steps, has_prev, *refs):
    place_ref, count_ref, code_ref, perms_ref, mii, mib, mbb, psi, phi = refs[:9]
    refs = refs[9 + has_prev:]
    coupling_out = refs[0]
    messages = refs[1:1 + inner]
    psi_acc, cross_acc, phi_acc = refs[1 + inner:]
    step = pl.program_id(0)
    used = slot < count_ref[0]
    block = mii.shape[1]

    @pl.when(used)
    def _():
        product = mm(mii[0], psi[0], ((1,), (0,))).astype(BF16)
        here = psi[0, pl.ds(pl.multiple_of(step * block, block), block), :]
        ib = mib[0]
        modes = phi[0]
        first = mm(here, product, ((0,), (0,)))
        second = mm(here, ib, ((0,), (0,)))
        third = mm(modes, product, ((0,), (0,))) + mm(modes, ib, ((0,), (0,)))

        @pl.when(step == 0)
        def _():
            psi_acc[...] = first
            cross_acc[...] = second
            phi_acc[...] = third

        @pl.when(step > 0)
        def _():
            psi_acc[...] += first
            cross_acc[...] += second
            phi_acc[...] += third

    @pl.when(step == steps - 1)
    def _():
        @pl.when(used)
        def _():
            coupling_out[0] = phi_acc[...]
            cross = cross_acc[...]
            reduced = psi_acc[...] + cross + cross.T + mbb[0].astype(F32)
            width = reduced.shape[0]
            row = perms_ref[pl.ds(slot, 1), :]
            pick = (lax.broadcasted_iota(jnp.int32, (width, width), 0) == row).astype(BF16)
            high, low = halves(reduced)
            high, low = halves(mm(pick, high, ((1,), (0,))) + mm(pick, low, ((1,), (0,))))
            psi_acc[...] = mm(high, pick, ((1,), (1,))) + mm(low, pick, ((1,), (1,)))

        @pl.when(jnp.logical_not(used))
        def _():
            coupling_out[0] = jnp.zeros_like(phi_acc)
            psi_acc[...] = jnp.zeros_like(psi_acc)

        mine = place_ref[0] % inner
        for q in range(inner):
            dest = mine ^ q
            for z in range(outer):
                start = pl.multiple_of((z * inner + dest) * rows, rows)
                messages[q][z * rows:(z + 1) * rows, :] = psi_acc[pl.ds(start, rows), :]
            if slot == 0:
                lane = lax.broadcasted_iota(jnp.int32, (META, psi_acc.shape[1]), 1)
                meta = jnp.zeros((META, psi_acc.shape[1]), F32)
                for j in range(code_ref.shape[0]):
                    meta = jnp.where(lane == j, code_ref[j].astype(F32), meta)
                messages[q][outer * rows:, :] = meta


def run_slot(slot, inner, outer, place, counts, block_map, arrays, prev):
    perms, mass_ii, mass_ib, mass_bb, psi, phi = arrays
    slots, size, width = psi.shape
    modes = phi.shape[2]
    rows = width // (inner * outer)
    block = min(256, size)
    steps = size // block
    smem = pl.BlockSpec(memory_space=pltpu.SMEM)
    tall = outer * rows + (META if slot == 0 else 0)
    in_specs = [
        smem,
        smem,
        smem,
        pl.BlockSpec(perms.shape, lambda i: (0, 0)),
        pl.BlockSpec((1, block, size), lambda i: (slot, i, 0)),
        pl.BlockSpec((1, block, width), lambda i: (slot, i, 0)),
        pl.BlockSpec((1, width, width), lambda i: (slot, 0, 0)),
        pl.BlockSpec((1, size, width), lambda i: (slot, 0, 0)),
        pl.BlockSpec((1, block, modes), lambda i: (slot, i, 0)),
    ]
    operands = [place, counts, block_map, perms, mass_ii, mass_ib, mass_bb, psi, phi]
    aliases = {}
    if prev is not None:
        in_specs.append(pl.BlockSpec(memory_space=pl.ANY))
        operands.append(prev)
        aliases = {9: 0}
    out = pl.pallas_call(
        functools.partial(slot_body, slot, inner, outer, rows, steps, int(prev is not None)),
        grid=(steps,),
        in_specs=in_specs,
        out_specs=[pl.BlockSpec((1, modes, width), lambda i: (slot, 0, 0))]
        + [pl.BlockSpec((tall, width), lambda i: (0, 0))] * inner,
        out_shape=[jax.ShapeDtypeStruct((slots, modes, width), F32)]
        + [jax.ShapeDtypeStruct((tall, width), F32)] * inner,
        scratch_shapes=[
            pltpu.VMEM((width, width), F32),
            pltpu.VMEM((width, width), F32),
            pltpu.VMEM((modes, width), F32),
        ],
        input_output_aliases=aliases,
        cost_estimate=pl.CostEstimate(
            flops=2 * size * width * (size + 2 * width + 2 * modes), bytes_accessed=3400000, transcendentals=0
        ),
        name=f"slot{slot}",
    )(*operands)
    return out[0], out[1:]


def repack_body(inner, outer, rows, meta, *refs):
    place_ref = refs[0]
    sources = refs[1:1 + inner]
    outs = refs[1 + inner:]
    mine = place_ref[0] // inner
    for k in range(outer):
        start = pl.multiple_of((mine ^ k) * rows, rows)
        for q in range(inner):
            outs[k][q * rows:(q + 1) * rows, :] = sources[q][pl.ds(start, rows), :]
            if meta:
                outs[k][inner * rows + q:inner * rows + q + 1, :] = sources[q][outer * rows:outer * rows + 1, :]


def repack(slot, inner, outer, rows, place, sources):
    width = sources[0].shape[1]
    tall = inner * rows + (META if slot == 0 else 0)
    return pl.pallas_call(
        functools.partial(repack_body, inner, outer, rows, slot == 0),
        in_specs=[pl.BlockSpec(memory_space=pltpu.SMEM)]
        + [pl.BlockSpec(memory_space=pltpu.VMEM)] * inner,
        out_specs=[pl.BlockSpec(memory_space=pltpu.VMEM)] * outer,
        out_shape=[jax.ShapeDtypeStruct((tall, width), F32)] * outer,
        name=f"repack{slot}",
    )(place, *sources)


def combine_body(inner, outer, rows, slots, codes_ref, *refs):
    sources = refs[:slots * outer]
    home, ahead = refs[slots * outer:]
    home[...] = jnp.zeros_like(home)
    ahead[...] = jnp.zeros_like(ahead)
    for j in range(slots):
        for k in range(outer):
            for q in range(inner):
                code = codes_ref[(k * inner + q) * slots + j]
                piece = sources[j * outer + k][q * rows:(q + 1) * rows, :]
                at = code % NBG

                @pl.when(code < NBG)
                def _():
                    home[at] += piece

                @pl.when(code >= NBG)
                def _():
                    ahead[at] += piece


def combine(inner, outer, rows, slots, codes, sources):
    width = sources[0].shape[1]
    vmem = pl.BlockSpec(memory_space=pltpu.VMEM)
    return pl.pallas_call(
        functools.partial(combine_body, inner, outer, rows, slots),
        in_specs=[pl.BlockSpec(memory_space=pltpu.SMEM)] + [vmem] * len(sources),
        out_specs=[vmem, vmem],
        out_shape=[jax.ShapeDtypeStruct((NBG, rows, width), F32)] * 2,
        name="combine",
    )(codes, *sources)


def per_device(counts, block_map, perms, mass_ii, mass_ib, mass_bb, constraint_modes, fixed_modes):
    slots = mass_ii.shape[0]
    width = mass_bb.shape[1]
    sub_size = lax.axis_size("sub")
    outer = OUTER
    inner = sub_size // outer
    rows = width // sub_size
    place = lax.axis_index("sub").astype(jnp.int32).reshape(1)
    arrays = (perms, mass_ii, mass_ib, mass_bb, constraint_modes, fixed_modes)

    coupling = None
    final = []
    for slot in range(slots):
        coupling, messages = run_slot(slot, inner, outer, place, counts, block_map, arrays, coupling)
        gathered = [messages[0]] + [crossed(messages[q], q) for q in range(1, inner)]
        packed = repack(slot, inner, outer, rows, place, gathered)
        final += [packed[0]] + [crossed(packed[k], k * inner) for k in range(1, outer)]
    metas = [final[k][inner * rows:inner * rows + inner, :slots] for k in range(outer)]
    codes = jnp.stack(metas).astype(jnp.int32).reshape(-1)
    home, ahead = combine(inner, outer, rows, slots, codes, final)
    return (home + shifted(ahead, "grp", 1), coupling)


def solution(mesh):
    placed = (
        P(("grp", "sub")),
        P(("grp", "sub")),
        P(("grp", "sub"), None),
        P(("grp", "sub"), None, None),
        P(("grp", "sub"), None, None),
        P(("grp", "sub"), None, None),
        P(("grp", "sub"), None, None),
        P(("grp", "sub"), None, None),
    )
    return jax.shard_map(
        per_device,
        mesh=mesh,
        in_specs=placed,
        out_specs=(P("grp", "sub", None), P(("grp", "sub"), None, None)),
        check_vma=False,
    )
```

```python
import functools

import jax
import jax.numpy as jnp
from jax import lax
from jax.experimental import pallas as pl
from jax.experimental.pallas import tpu as pltpu
from jax.sharding import PartitionSpec as P

NBG = 16
OUTER = 4
META = 8
F32 = jnp.float32
BF16 = jnp.bfloat16


def shifted(value, axis, by):
    peers = lax.axis_size(axis)
    return lax.ppermute(value, axis, [(i, (i + by) % peers) for i in range(peers)])


def crossed(value, mask):
    peers = lax.axis_size("sub")
    return lax.ppermute(value, "sub", [(i, i ^ mask) for i in range(peers)])


def mm(left, right, dims):
    return lax.dot_general(left, right, (dims, ((), ())), preferred_element_type=F32)


def halves(value):
    high = value.astype(BF16)
    return high, (value - high.astype(F32)).astype(BF16)


def in_vmem(value):
    return pltpu.with_memory_space_constraint(value, pltpu.VMEM)


def slot_body(group, last, inner, outer, rows, chunks, extra, *refs):
    place_ref, count_ref, code_ref, perms_ref, mii, mib, mbb, psi, phi = refs[:9]
    refs = refs[9 + extra:]
    coupling_out = refs[0]
    scratch = refs[len(refs) - 10:]
    messages = list(refs[1:len(refs) - 10])
    mii_v, mib_v, mbb_v, psi_v, phi_v, product_v, place_v, coupled_v, sems, out_sems = scratch
    size = psi_v.shape[1]
    block = size // chunks
    plans = []
    for n, slot in enumerate(group):
        loads = [pltpu.make_async_copy(psi.at[slot], psi_v.at[n], sems.at[n, 0])]
        for c in range(chunks):
            part = pl.ds(c * block, block)
            loads.append(pltpu.make_async_copy(mii.at[slot, part], mii_v.at[n, part], sems.at[n, 1 + c]))
        others = ((mib, mib_v), (mbb, mbb_v), (phi, phi_v))
        for m, (source, target) in enumerate(others):
            loads.append(pltpu.make_async_copy(source.at[slot], target.at[n], sems.at[n, 1 + chunks + m]))
        plans.append(loads)

        @pl.when(slot < count_ref[0])
        def _():
            for load in loads:
                load.start()

    saves = []
    for n, slot in enumerate(group):
        loads = plans[n]
        used = slot < count_ref[0]

        @pl.when(used)
        def _():
            loads[0].wait()
            for c in range(chunks):
                loads[1 + c].wait()
                part = pl.ds(c * block, block)
                product_v[part, :] = mm(mii_v[n, part, :], psi_v[n], ((1,), (0,))).astype(BF16)
            reduced = mm(psi_v[n], product_v[...], ((0,), (0,)))
            loads[1 + chunks].wait()
            place_v[...] = mm(psi_v[n], mib_v[n], ((0,), (0,)))
            loads[2 + chunks].wait()
            reduced = reduced + place_v[...] + place_v[...].T + mbb_v[n].astype(F32)
            width = reduced.shape[0]
            row = perms_ref[pl.ds(slot, 1), :]
            pick = (lax.broadcasted_iota(jnp.int32, (width, width), 0) == row).astype(BF16)
            high, low = halves(reduced)
            high, low = halves(mm(pick, high, ((1,), (0,))) + mm(pick, low, ((1,), (0,))))
            place_v[...] = mm(high, pick, ((1,), (1,))) + mm(low, pick, ((1,), (1,)))
            loads[3 + chunks].wait()
            modes = phi_v[n]
            coupled_v[n] = mm(modes, product_v[...], ((0,), (0,))) + mm(modes, mib_v[n], ((0,), (0,)))

        @pl.when(jnp.logical_not(used))
        def _():
            coupled_v[n] = jnp.zeros(coupled_v.shape[1:], F32)
            place_v[...] = jnp.zeros_like(place_v)

        save = pltpu.make_async_copy(coupled_v.at[n], coupling_out.at[slot], out_sems.at[n])
        save.start()
        saves.append(save)
        if slot < last:
            mine = place_ref[0] // inner
            tall = inner * rows
            for k in range(outer):
                start = pl.multiple_of((mine ^ k) * tall, rows)
                message = messages.pop(0)
                message[:tall, :] = place_v[pl.ds(start, tall), :]
                if slot == 0:
                    lane = lax.broadcasted_iota(jnp.int32, (META, place_v.shape[1]), 1)
                    meta = jnp.zeros((META, place_v.shape[1]), F32)
                    for j in range(code_ref.shape[0]):
                        meta = jnp.where(lane == j, code_ref[j].astype(F32), meta)
                    message[tall:, :] = meta
        else:
            mine = place_ref[0] % inner
            for q in range(inner):
                message = messages.pop(0)
                for z in range(outer):
                    start = pl.multiple_of((z * inner + (mine ^ q)) * rows, rows)
                    message[z * rows:(z + 1) * rows, :] = place_v[pl.ds(start, rows), :]
    for save in saves:
        save.wait()


def run_slots(group, inner, outer, place, counts, block_map, arrays, prev):
    perms, mass_ii, mass_ib, mass_bb, psi, phi = arrays
    slots, size, width = psi.shape
    modes = phi.shape[2]
    rows = width // (inner * outer)
    chunks = 2
    held = len(group)
    smem = pl.BlockSpec(memory_space=pltpu.SMEM)
    vmem = pl.BlockSpec(memory_space=pltpu.VMEM)
    whole = pl.BlockSpec(memory_space=pl.ANY)
    tails = []
    for slot in group:
        if slot < slots - 1:
            tails += [inner * rows + (META if slot == 0 else 0)] * outer
        else:
            tails += [outer * rows] * inner
    in_specs = [smem, smem, smem, vmem] + [whole] * 5
    operands = [place, counts, block_map, perms, mass_ii, mass_ib, mass_bb, psi, phi]
    aliases = {}
    if prev is not None:
        aliases = {9: 0}
        operands.append(prev)
        in_specs.append(whole)
    out = pl.pallas_call(
        functools.partial(slot_body, group, slots - 1, inner, outer, rows, chunks, len(operands) - 9),
        in_specs=in_specs,
        out_specs=[whole] + [vmem] * len(tails),
        out_shape=[jax.ShapeDtypeStruct((slots, modes, width), F32)]
        + [pltpu.VMEM((tall, width), F32) for tall in tails],
        scratch_shapes=[
            pltpu.VMEM((held, size, size), BF16),
            pltpu.VMEM((held, size, width), BF16),
            pltpu.VMEM((held, width, width), BF16),
            pltpu.VMEM((held, size, width), BF16),
            pltpu.VMEM((held, size, modes), BF16),
            pltpu.VMEM((size, width), BF16),
            pltpu.VMEM((width, width), F32),
            pltpu.VMEM((held, modes, width), F32),
            pltpu.SemaphoreType.DMA((held, chunks + 4)),
            pltpu.SemaphoreType.DMA((held,)),
        ],
        input_output_aliases=aliases,
        cost_estimate=pl.CostEstimate(
            flops=2 * held * size * width * (size + 2 * width + 2 * modes),
            bytes_accessed=3400000 * held,
            transcendentals=0,
        ),
        name=f"slots{group[0]}",
    )(*operands)
    return out[0], out[1:]


def repack_body(mine, near, far, rows, meta, extra, *refs):
    place_ref = refs[0]
    sources = refs[1:1 + near]
    outs = refs[1 + near + extra:]
    own = mine(place_ref[0])
    for k in range(far):
        start = pl.multiple_of((own ^ k) * rows, rows)
        for q in range(near):
            outs[k][q * rows:(q + 1) * rows, :] = sources[q][pl.ds(start, rows), :]
            if meta:
                outs[k][near * rows + q:near * rows + q + 1, :] = sources[q][far * rows:far * rows + 1, :]


def repack(slot, mine, near, far, rows, place, sources, after):
    width = sources[0].shape[1]
    tall = near * rows + (META if slot == 0 else 0)
    vmem = pl.BlockSpec(memory_space=pltpu.VMEM)
    return pl.pallas_call(
        functools.partial(repack_body, mine, near, far, rows, slot == 0, len(after)),
        in_specs=[pl.BlockSpec(memory_space=pltpu.SMEM)]
        + [vmem] * near
        + [pl.BlockSpec(memory_space=pl.ANY)] * len(after),
        out_specs=[vmem] * far,
        out_shape=[pltpu.VMEM((tall, width), F32)] * far,
        name=f"repack{slot}",
    )(place, *[in_vmem(source) for source in sources], *after)


def combine_body(inner, outer, rows, slots, codes_ref, *refs):
    home, ahead = refs[len(refs) - 2:]
    sources = list(refs[:len(refs) - 2])
    home[...] = jnp.zeros_like(home)
    ahead[...] = jnp.zeros_like(ahead)
    for j in range(slots):
        far, near = (inner, outer) if j < slots - 1 else (outer, inner)
        for m in range(far):
            source = sources.pop(0)
            for n in range(near):
                q, k = (m, n) if j < slots - 1 else (n, m)
                code = codes_ref[(q * outer + k) * slots + j]
                piece = source[n * rows:(n + 1) * rows, :]
                at = code % NBG

                @pl.when(code < NBG)
                def _():
                    home[at] += piece

                @pl.when(code >= NBG)
                def _():
                    ahead[at] += piece


def combine(inner, outer, rows, slots, codes, sources):
    width = sources[0].shape[1]
    vmem = pl.BlockSpec(memory_space=pltpu.VMEM)
    return pl.pallas_call(
        functools.partial(combine_body, inner, outer, rows, slots),
        in_specs=[pl.BlockSpec(memory_space=pltpu.SMEM)] + [vmem] * len(sources),
        out_specs=[vmem, vmem],
        out_shape=[pltpu.VMEM((NBG, rows, width), F32)] * 2,
        name="combine",
    )(codes, *[in_vmem(source) for source in sources])


def per_device(counts, block_map, perms, mass_ii, mass_ib, mass_bb, constraint_modes, fixed_modes):
    slots = mass_ii.shape[0]
    width = mass_bb.shape[1]
    sub_size = lax.axis_size("sub")
    outer = OUTER
    inner = sub_size // outer
    rows = width // sub_size
    place = lax.axis_index("sub").astype(jnp.int32).reshape(1)
    arrays = (perms, mass_ii, mass_ib, mass_bb, constraint_modes, fixed_modes)

    def across(pieces, stride):
        return [pieces[0]] + [crossed(pieces[k], k * stride) for k in range(1, len(pieces))]

    coupling, leaving = run_slots((0,), inner, outer, place, counts, block_map, arrays, None)
    first = across(leaving, inner)
    later = tuple(range(1, slots))
    coupling, leaving = run_slots(later, inner, outer, place, counts, block_map, arrays, coupling)
    arrived = [first]
    for slot in later[:-1]:
        arrived.append(across(leaving[(slot - 1) * outer:slot * outer], inner))
    arrived.append(across(leaving[(slots - 2) * outer:], 1))

    final = [None] * slots
    after = []
    for slot in [0, slots - 1] + list(later[:-1]):
        if slot < slots - 1:
            packed = repack(slot, lambda at: at % inner, outer, inner, rows, place, arrived[slot], after)
            final[slot] = across(packed, 1)
        else:
            packed = repack(slot, lambda at: at // inner, inner, outer, rows, place, arrived[slot], after)
            final[slot] = across(packed, inner)
        after = [packed[1]]
    metas = [final[0][q][outer * rows:outer * rows + outer, :slots] for q in range(inner)]
    codes = jnp.stack(metas).astype(jnp.int32).reshape(-1)
    final = [message for group in final for message in group]
    home, ahead = combine(inner, outer, rows, slots, codes, final)
    return (home + shifted(ahead, "grp", 1), coupling)


def solution(mesh):
    placed = (
        P(("grp", "sub")),
        P(("grp", "sub")),
        P(("grp", "sub"), None),
        P(("grp", "sub"), None, None),
        P(("grp", "sub"), None, None),
        P(("grp", "sub"), None, None),
        P(("grp", "sub"), None, None),
        P(("grp", "sub"), None, None),
    )
    return jax.shard_map(
        per_device,
        mesh=mesh,
        in_specs=placed,
        out_specs=(P("grp", "sub", None), P(("grp", "sub"), None, None)),
        check_vma=False,
    )
```

```python
import functools

import jax
import jax.numpy as jnp
from jax import lax
from jax.experimental import pallas as pl
from jax.experimental.pallas import tpu as pltpu
from jax.sharding import PartitionSpec as P

NBG = 16
OUTER = 4
META = 8
F32 = jnp.float32
BF16 = jnp.bfloat16


def shifted(value, axis, by):
    peers = lax.axis_size(axis)
    return lax.ppermute(value, axis, [(i, (i + by) % peers) for i in range(peers)])


def crossed(value, mask):
    peers = lax.axis_size("sub")
    return lax.ppermute(value, "sub", [(i, i ^ mask) for i in range(peers)])


def mm(left, right, dims):
    return lax.dot_general(left, right, (dims, ((), ())), preferred_element_type=F32)


def halves(value):
    high = value.astype(BF16)
    return high, (value - high.astype(F32)).astype(BF16)


def in_vmem(value):
    return pltpu.with_memory_space_constraint(value, pltpu.VMEM)


def slots_body(inner, outer, rows, chunks, *refs):
    place_ref, count_ref, code_ref, perms, mii, mib, mbb, psi, phi, coupling_out = refs[:10]
    straight = refs[10:10 + outer]
    turned = refs[10 + outer:10 + outer + inner]
    scratch = refs[10 + outer + inner:]
    perms_v, mii_v, mib_v, mbb_v, psi_v, phi_v, product_v, place_v, coupled_v, sems, row_sem, out_sems = scratch
    slots, size, width = psi_v.shape
    half = width // 2
    block = size // chunks
    plans = []
    rows_in = pltpu.make_async_copy(perms, perms_v, row_sem)
    for slot in range(slots):
        loads = [pltpu.make_async_copy(psi.at[slot], psi_v.at[slot], sems.at[slot, 0])]
        for c in range(chunks):
            part = pl.ds(c * block, block)
            loads.append(pltpu.make_async_copy(mii.at[slot, part], mii_v.at[slot, part], sems.at[slot, 1 + c]))
        others = ((mib, mib_v), (phi, phi_v), (mbb, mbb_v))
        for m, (source, target) in enumerate(others):
            loads.append(pltpu.make_async_copy(source.at[slot], target.at[slot], sems.at[slot, 1 + chunks + m]))
        for load in loads:
            load.start()
        if slot == 0:
            rows_in.start()
        plans.append(loads)

    place = place_ref[0]
    lane = lax.broadcasted_iota(jnp.int32, (META, half), 1)
    meta = jnp.zeros((META, half), F32)
    for slot in range(slots):
        meta = jnp.where(lane == slot, code_ref[slot].astype(F32), meta)
    for k in range(outer):
        straight[k][slots * inner * rows:, :] = meta

    saves = []
    for slot in range(slots):
        loads = plans[slot]
        used = slot < count_ref[0]
        save = pltpu.make_async_copy(coupled_v.at[slot], coupling_out.at[slot], out_sems.at[slot])
        saves.append(save)
        for load in loads:
            load.wait() if slot > 0 else None
        if slot == 0:
            loads[0].wait()
            loads[1].wait()

        @pl.when(used)
        def _():
            for c in range(chunks):
                if slot == 0 and c > 0:
                    loads[1 + c].wait()
                part = pl.ds(c * block, block)
                product_v[part, :] = mm(mii_v[slot, part, :], psi_v[slot], ((1,), (0,))).astype(BF16)

        if slot == 0:

            @pl.when(jnp.logical_not(used))
            def _():
                for c in range(1, chunks):
                    loads[1 + c].wait()

            for load in loads[1 + chunks:]:
                load.wait()
            rows_in.wait()

        @pl.when(used)
        def _():
            modes = phi_v[slot]
            coupled_v[slot] = mm(modes, product_v[...], ((0,), (0,))) + mm(modes, mib_v[slot], ((0,), (0,)))
            save.start()
            reduced = mm(psi_v[slot], product_v[...], ((0,), (0,)))
            place_v[...] = mm(psi_v[slot], mib_v[slot], ((0,), (0,)))
            reduced = reduced + place_v[...] + place_v[...].T + mbb_v[slot].astype(F32)
            row = perms_v[pl.ds(slot, 1), :]
            pick = (lax.broadcasted_iota(jnp.int32, (width, width), 0) == row).astype(BF16)
            high, low = halves(reduced)
            high, low = halves(mm(pick, high, ((1,), (0,))) + mm(pick, low, ((1,), (0,))))
            place_v[...] = mm(high, pick, ((1,), (1,))) + mm(low, pick, ((1,), (1,)))

        @pl.when(jnp.logical_not(used))
        def _():
            coupled_v[slot] = jnp.zeros(coupled_v.shape[1:], F32)
            save.start()
            place_v[...] = jnp.zeros_like(place_v)

        tall = inner * rows
        for k in range(outer):
            start = pl.multiple_of(((place // inner) ^ k) * tall, rows)
            straight[k][slot * tall:(slot + 1) * tall, :] = place_v[pl.ds(start, tall), :half]
        for q in range(inner):
            for z in range(outer):
                start = pl.multiple_of((z * inner + ((place % inner) ^ q)) * rows, rows)
                at = (slot * outer + z) * rows
                turned[q][at:at + rows, :] = place_v[pl.ds(start, rows), half:]
    for save in saves:
        save.wait()


def run_slots(inner, outer, place, counts, block_map, perms, mass_ii, mass_ib, mass_bb, psi, phi):
    slots, size, width = psi.shape
    modes = phi.shape[2]
    half = width // 2
    rows = width // (inner * outer)
    chunks = 2
    smem = pl.BlockSpec(memory_space=pltpu.SMEM)
    vmem = pl.BlockSpec(memory_space=pltpu.VMEM)
    whole = pl.BlockSpec(memory_space=pl.ANY)
    talls = [slots * inner * rows + META] * outer + [slots * outer * rows] * inner
    out = pl.pallas_call(
        functools.partial(slots_body, inner, outer, rows, chunks),
        in_specs=[smem] * 3 + [whole] * 6,
        out_specs=[whole] + [vmem] * len(talls),
        out_shape=[jax.ShapeDtypeStruct((slots, modes, width), F32)]
        + [pltpu.VMEM((tall, half), F32) for tall in talls],
        scratch_shapes=[
            pltpu.VMEM(perms.shape, jnp.int32),
            pltpu.VMEM((slots, size, size), BF16),
            pltpu.VMEM((slots, size, width), BF16),
            pltpu.VMEM((slots, width, width), BF16),
            pltpu.VMEM((slots, size, width), BF16),
            pltpu.VMEM((slots, size, modes), BF16),
            pltpu.VMEM((size, width), BF16),
            pltpu.VMEM((width, width), F32),
            pltpu.VMEM((slots, modes, width), F32),
            pltpu.SemaphoreType.DMA((slots, chunks + 4)),
            pltpu.SemaphoreType.DMA,
            pltpu.SemaphoreType.DMA((slots,)),
        ],
        name="slots",
    )(place, counts, block_map, perms, mass_ii, mass_ib, mass_bb, psi, phi)
    return out[0], out[1:1 + outer], out[1 + outer:]


def repack_body(mine, near, far, slots, rows, meta, extra, *refs):
    place_ref = refs[0]
    sources = refs[1:1 + near]
    outs = refs[1 + near + extra:]
    own = mine(place_ref[0])
    for k in range(far):
        for q in range(near):
            for j in range(slots):
                start = pl.multiple_of((j * far + (own ^ k)) * rows, rows)
                at = (j * near + q) * rows
                outs[k][at:at + rows, :] = sources[q][pl.ds(start, rows), :]
            if meta:
                at = slots * near * rows + q
                end = slots * far * rows
                outs[k][at:at + 1, :] = sources[q][end:end + 1, :]


def repack(name, mine, near, far, slots, rows, meta, place, sources, after):
    width = sources[0].shape[1]
    tall = slots * near * rows + meta
    vmem = pl.BlockSpec(memory_space=pltpu.VMEM)
    return pl.pallas_call(
        functools.partial(repack_body, mine, near, far, slots, rows, meta > 0, len(after)),
        in_specs=[pl.BlockSpec(memory_space=pltpu.SMEM)]
        + [vmem] * near
        + [pl.BlockSpec(memory_space=pl.ANY)] * len(after),
        out_specs=[vmem] * far,
        out_shape=[pltpu.VMEM((tall, width), F32)] * far,
        name=name,
    )(place, *[in_vmem(source) for source in sources], *after)


def combine_body(index, near, far, slots, rows, codes_ref, *refs):
    sources = refs[:far]
    home, ahead = refs[len(refs) - 2:]
    home[...] = jnp.zeros_like(home)
    ahead[...] = jnp.zeros_like(ahead)
    for m in range(far):
        for j in range(slots):
            for n in range(near):
                code = codes_ref[index(m, n) * slots + j]
                at = (j * near + n) * rows
                piece = sources[m][at:at + rows, :]
                block = code % NBG

                @pl.when(code < NBG)
                def _():
                    home[block] += piece

                @pl.when(code >= NBG)
                def _():
                    ahead[block] += piece


def combine(name, index, near, slots, rows, codes, sources, after):
    width = sources[0].shape[1]
    vmem = pl.BlockSpec(memory_space=pltpu.VMEM)
    return pl.pallas_call(
        functools.partial(combine_body, index, near, len(sources), slots, rows),
        in_specs=[pl.BlockSpec(memory_space=pltpu.SMEM)]
        + [vmem] * len(sources)
        + [pl.BlockSpec(memory_space=pl.ANY)] * len(after),
        out_specs=[vmem, vmem],
        out_shape=[pltpu.VMEM((NBG, rows, width), F32)] * 2,
        name=name,
    )(codes, *[in_vmem(source) for source in sources], *after)


def per_device(counts, block_map, perms, mass_ii, mass_ib, mass_bb, constraint_modes, fixed_modes):
    slots = mass_ii.shape[0]
    width = mass_bb.shape[1]
    sub_size = lax.axis_size("sub")
    outer = OUTER
    inner = sub_size // outer
    rows = width // sub_size
    place = lax.axis_index("sub").astype(jnp.int32).reshape(1)

    def across(pieces, stride):
        return [pieces[0]] + [crossed(pieces[k], k * stride) for k in range(1, len(pieces))]

    coupling, straight, turned = run_slots(
        inner, outer, place, counts, block_map, perms, mass_ii, mass_ib, mass_bb, constraint_modes, fixed_modes
    )
    left = across(straight, inner)
    right = across(turned, 1)
    right = repack("right", lambda at: at // inner, inner, outer, slots, rows, 0, place, right, [])
    after = [right[1]]
    right = across(right, inner)
    left = repack("left", lambda at: at % inner, outer, inner, slots, rows, META, place, left, after)
    left = across(left, 1)
    end = slots * outer * rows
    codes = jnp.stack([left[q][end:end + outer, :slots] for q in range(inner)])
    codes = codes.astype(jnp.int32).reshape(-1)
    home_left, ahead_left = combine("sum_left", lambda m, n: m * outer + n, outer, slots, rows, codes, left, [])
    far_left = shifted(ahead_left, "grp", 1)
    home_right, ahead_right = combine(
        "sum_right", lambda m, n: n * outer + m, inner, slots, rows, codes, right, [ahead_left]
    )
    far_right = shifted(ahead_right, "grp", 1)
    blocks = jnp.concatenate([home_left + far_left, home_right + far_right], axis=2)
    return (blocks, coupling)


def solution(mesh):
    placed = (
        P(("grp", "sub")),
        P(("grp", "sub")),
        P(("grp", "sub"), None),
        P(("grp", "sub"), None, None),
        P(("grp", "sub"), None, None),
        P(("grp", "sub"), None, None),
        P(("grp", "sub"), None, None),
        P(("grp", "sub"), None, None),
    )
    return jax.shard_map(
        per_device,
        mesh=mesh,
        in_specs=placed,
        out_specs=(P("grp", "sub", None), P(("grp", "sub"), None, None)),
        check_vma=False,
    )
```
